32 devices in a mesh: grp: 4 (over y, x), seq: 8 (over z, core).
Axes of the slice: x: 2, y: 2, z: 4, core: 2. Of those that a mesh axis runs over, the one named last changes fastest.
Arguments:
- tokens: bfloat16 [2048, 8192], P(None, 'seq'), may hold values from -16 to 16
- proj_weight: bfloat16 [8192, 5120], P('seq', 'grp'), may hold values from -0.0625 to 0.0625
- proj_bias: bfloat16 [5120], P('grp'), may hold values from -3 to 3
- out_weight: bfloat16 [4096, 8192], P('grp'), may hold values from -0.125 to 0.125
- doc_ids: int32 [2048], P('seq'), may hold values from 0 to 2, never falling along the last dimension, each value on 1 to 1280 neighbouring positions
Outputs:
- mixed: bfloat16 [2048, 8192], P('seq', 'grp')
The draws below stay inside these ranges and needn't reach their ends.
Inputs may be any that keep to these rules, and one draw needn't show every extreme that they name: `doc_ids`: numbers never fall along the sequence; every document has 1 to 1280 tokens, one exactly that many; every number up to 2 is used.
All inputs are finite; a program needn't handle non-finite values.
Results may differ from the reference program's by a relative error of at most 0.012.
Values may be sent and summed in bfloat16 or wider, within the bound.
A program may use at most 256 MiB of HBM per device.

```python
import math
import jax
import jax.numpy as jnp
import numpy as np
from jax import lax

D = 8192
Q_HEADS = 32
KV_HEADS = 4
HEAD_DIM = 128
TOK_DEV = 256
SPAN = 5
GQA = 8
TOKENS = 2048
DOCS = 3


def draw_tokens(key, part):
    normals = jax.random.normal(jax.random.fold_in(key, 11), (TOKENS, D), jnp.float32)
    block_offsets = jax.random.normal(jax.random.fold_in(key, 19), (TOKENS // TOK_DEV, D), jnp.float32)
    offset_rows = jnp.repeat(block_offsets, TOK_DEV, axis=0)
    result = jnp.clip(normals + 1.5 * offset_rows, -8.0, 8.0)
    return result.astype(jnp.bfloat16)


def with_spikes(drawn, own_key, source, target, shards_of, factor):
    owner, partner = [(jnp.arange(drawn.shape[position]) // (drawn.shape[position] // shards_of)).reshape([-1 if axis == position else 1 for axis in range(drawn.ndim)]) for position in (source, target)]
    chosen = jax.random.permutation(own_key, shards_of)[partner]
    strong = (owner == chosen) | (owner == (partner + shards_of // 2) % shards_of)
    return jnp.where(strong, factor * drawn, drawn)


def block_scale(own_key, extent, shards, low, largest):
    def one(axis_at, parts):
        draws = jax.random.uniform(jax.random.fold_in(jax.random.fold_in(own_key, 6), axis_at), (parts,), jnp.float32, low / len(shards), largest / len(shards))
        return jnp.repeat(jnp.exp(draws), extent[axis_at] // parts).reshape((-1,) + (1,) * (len(extent) - axis_at - 1))

    level = one(*shards[0])
    for cut in shards[1:]:
        level = level * one(*cut)
    return level


def split_up(number_of, total, limit, slope):
    weights = [(1 << 20) // math.isqrt(standing ** slope) + 1 for standing in range(2, number_of + 1)]
    spare, holding = total - limit - (number_of - 1), [1] * (number_of - 1)
    while spare > 0:
        movable = [i for i in range(number_of - 1) if holding[i] < limit]
        pool, remaining = sum([weights[i] for i in movable]), spare
        for i in movable:
            more = min(limit - holding[i], max(1, remaining * weights[i] // pool), spare)
            holding[i] = holding[i] + more
            spare = spare - more
    return np.array([limit] + holding)


def ragged_sizes(key, amount, total, limit, slope):
    if amount == 2:
        one = jax.random.randint(key, (), max(1, total - limit), min(limit, total - 1) + 1)
        return jnp.stack([one, total - one])
    sizes = jnp.asarray(split_up(amount, total, limit, slope), jnp.int32)
    twos = (amount - 1) // 2
    donor, sink = sizes[1:1 + 2 * twos:2], sizes[2:2 + 2 * twos:2]
    room = jnp.minimum(donor - 1, limit - sink)
    shifted = jax.random.randint(jax.random.fold_in(key, 1), (twos,), 0, 1 << 20) % (room + 1)
    sizes = sizes.at[1:1 + 2 * twos:2].set(donor - shifted).at[2:2 + 2 * twos:2].set(sink + shifted)
    return sizes[jax.random.permutation(jax.random.fold_in(key, 2), amount)]


def normal_values(rng, shape, scale, reach, split=(), held_as=jnp.bfloat16):
    drawn = jax.random.normal(rng, shape, jnp.float32) * scale
    if len(split) > 0:
        drawn = block_scale(rng, shape, split, -0.22, 0.18) * drawn
    return jnp.clip(drawn, min=-reach, max=reach).astype(held_as)


def bell_draw_with(own_key, extent, deviation, limit, split, heavy, kind=jnp.bfloat16):
    array = deviation * jax.random.normal(own_key, extent, jnp.float32)
    if split:
        array = array * block_scale(own_key, extent, split, -0.22, 0.18)
    return jnp.clip(with_spikes(array, jax.random.fold_in(own_key, 3), *heavy), -limit, limit).astype(kind)


def setup_inputs(seed: int = 0) -> dict:
    splits = jax.random.split(jax.random.key(seed), 6)
    tokens = draw_tokens(jax.random.fold_in(splits[5], 71), 0)
    proj_weight = normal_values(splits[1], (D, KV_HEADS * (GQA + 2) * HEAD_DIM), D ** -0.5, 0.0625, ((0, 8), (1, 4)))
    proj_bias = normal_values(splits[2], (KV_HEADS * (GQA + 2) * HEAD_DIM,), 0.5, 3.0, ((0, 4),))
    out_weight = bell_draw_with(splits[3], (Q_HEADS * HEAD_DIM, D), (Q_HEADS * HEAD_DIM) ** -0.5, 0.125, ((0, 4),), (0, 1, 4, 2.0))
    doc_ids = jnp.searchsorted(jnp.cumsum(ragged_sizes(splits[4], DOCS, TOKENS, SPAN * TOK_DEV, 1)), jnp.arange(TOKENS), side="right").astype(jnp.int32)
    return dict(tokens=tokens, proj_weight=proj_weight, proj_bias=proj_bias, out_weight=out_weight, doc_ids=doc_ids)


theta_base = 1000000.0


def rotate(inputs, positions, head_dim):
    half_dim = head_dim // 2
    inverse_freq = theta_base ** (-(jnp.arange(half_dim, dtype=jnp.float32) * 2.0) / head_dim)
    angles = positions.astype(jnp.float32)[:, None] * inverse_freq[None, :]
    cosine = jnp.concatenate([jnp.cos(angles), jnp.cos(angles)], axis=1)
    sine_table = jnp.concatenate([jnp.sin(angles), jnp.sin(angles)], axis=1)
    low_half = inputs[..., :half_dim]
    high_half = inputs[..., half_dim:]
    turned = jnp.concatenate([-high_half, low_half], axis=-1)
    return inputs * cosine[:, None, :] + turned * sine_table[:, None, :]


def reference(tokens, proj_weight, proj_bias, out_weight, doc_ids):
    projected = jnp.dot(tokens, proj_weight, preferred_element_type=jnp.float32) + proj_bias.astype(jnp.float32)[None, :]
    projected = projected.reshape(TOKENS, KV_HEADS, GQA + 2, HEAD_DIM)
    positions = jnp.arange(TOKENS, dtype=jnp.int32)
    queries = rotate(projected[:, :, :GQA, :].reshape(TOKENS, Q_HEADS, HEAD_DIM), positions, HEAD_DIM).astype(jnp.bfloat16)
    key_rows = rotate(projected[:, :, GQA, :], positions, HEAD_DIM).astype(jnp.bfloat16)
    value_rows = projected[:, :, GQA + 1, :].astype(jnp.bfloat16)
    allowed = (doc_ids[None, :] == doc_ids[:, None]) & (positions[None, :] <= positions[:, None])
    score_scale = HEAD_DIM ** -0.5

    def one_head(head_index):
        query_head = lax.dynamic_index_in_dim(queries, head_index, 1, keepdims=False).astype(jnp.float32)
        key_head = lax.dynamic_index_in_dim(key_rows, head_index // GQA, 1, keepdims=False).astype(jnp.float32)
        value_head = lax.dynamic_index_in_dim(value_rows, head_index // GQA, 1, keepdims=False)
        scores = jnp.dot(query_head, key_head.T, preferred_element_type=jnp.float32) * score_scale
        scores = jnp.where(allowed, scores, -jnp.inf)
        row_max = jnp.max(scores, axis=1, keepdims=True)
        weights = jnp.exp(scores - row_max)
        row_sum = jnp.sum(weights, axis=1, keepdims=True)
        summed = jnp.dot(weights.astype(jnp.bfloat16), value_head, preferred_element_type=jnp.float32)
        return (summed / row_sum).astype(jnp.bfloat16)

    head_outputs = lax.map(one_head, jnp.arange(Q_HEADS, dtype=jnp.int32))
    attended = jnp.transpose(head_outputs, (1, 0, 2)).reshape(TOKENS, Q_HEADS * HEAD_DIM)
    return jnp.dot(attended, out_weight, preferred_element_type=jnp.float32).astype(jnp.bfloat16)
```

```python
import functools

import jax
import jax.numpy as jnp
from jax import lax
from jax.experimental import pallas as pl
from jax.experimental.pallas import tpu as pltpu
from jax.sharding import PartitionSpec as P

HEAD_DIM = 128
GQA = 8
MESH = pl.DeviceIdType.MESH

theta_base = 1000000.0
neg_large = -1e30


def rope_tables(positions, head_dim):
    half_dim = head_dim // 2
    inverse_freq = theta_base ** (-(jnp.arange(half_dim, dtype=jnp.float32) * 2.0) / head_dim)
    angles = positions.astype(jnp.float32)[:, None] * inverse_freq[None, :]
    cosine, sine = jnp.cos(angles), jnp.sin(angles)
    return jnp.concatenate([cosine, cosine], axis=1), jnp.concatenate([-sine, sine], axis=1)


def proj_kernel(
    line, chunks, rows, width,
    tok_ref, w_ref, bias_ref, cos_ref, sin_ref, ids_ref,
    q_ref, kv_ref, idall_ref,
    pair_out, pair_in, up_in, dn_in, total,
    pair_ss, pair_rs, line_ss, up_rs, dn_rs, id_ss, id_rs, kvl_ss, kvl_rs, kvp_ss, kvp_rs,
):
    g = lax.axis_index("grp")
    s = lax.axis_index("seq")
    z, c = s // 2, lax.rem(s, 2)
    n = 2 * line
    partner = s + 1 - 2 * c
    low = z < line // 2

    barrier = pltpu.get_barrier_semaphore()
    for i in range(1, n):
        pl.semaphore_signal(barrier, inc=1, device_id=(g, lax.rem(s + i, n)), device_id_type=MESH)
    pl.semaphore_wait(barrier, n - 1)

    def id_copy(i):
        return pltpu.make_async_remote_copy(
            ids_ref, idall_ref.at[s], id_ss.at[i], id_rs.at[i],
            device_id=(g, lax.rem(s + i, n)), device_id_type=MESH,
        )

    def id_wait(i):
        return pltpu.make_async_remote_copy(
            ids_ref, idall_ref.at[lax.rem(s + n - i, n)], id_ss.at[i], id_rs.at[i],
            device_id=(g, lax.rem(s + i, n)), device_id_type=MESH,
        )

    idall_ref[s] = ids_ref[...]

    def offset(kk):
        return pl.multiple_of(lax.rem(kk + chunks - 1, chunks) * width, width)

    def product(kk, dest, core):
        row = pl.multiple_of((2 * dest + core) * rows, rows)
        return jnp.dot(
            tok_ref[pl.ds(row, rows), :], w_ref[:, pl.ds(offset(kk), width)],
            preferred_element_type=jnp.float32,
        )

    def pair_copy(kk, dest):
        return pltpu.make_async_remote_copy(
            pair_out.at[kk, dest], pair_in.at[kk, dest], pair_ss.at[kk, dest], pair_rs.at[kk, dest],
            device_id=(g, partner), device_id_type=MESH,
        )

    def up_copy(kk, dest):
        return pltpu.make_async_remote_copy(
            pair_in.at[kk, dest], up_in.at[kk, dest], line_ss.at[kk, dest], up_rs.at[kk, dest],
            device_id=(g, lax.rem(s + 2, n)), device_id_type=MESH,
        )

    def dn_copy(kk, dest):
        return pltpu.make_async_remote_copy(
            pair_in.at[kk, dest], dn_in.at[kk, dest], line_ss.at[kk, dest], dn_rs.at[kk, dest],
            device_id=(g, lax.rem(s + n - 2, n)), device_id_type=MESH,
        )

    def kv_line(zz):
        block = kv_ref.at[2 * zz + c]
        return pltpu.make_async_remote_copy(
            block, block, kvl_ss.at[zz], kvl_rs.at[zz], device_id=(g, lax.rem(s + 2, n)), device_id_type=MESH
        )

    def kv_pair(zz):
        block = kv_ref.at[2 * zz + c]
        return pltpu.make_async_remote_copy(
            block, block, kvp_ss.at[zz], kvp_rs.at[zz], device_id=(g, partner), device_id_type=MESH
        )

    def kv_pair_wait(zz):
        block = kv_ref.at[2 * zz + 1 - c]
        return pltpu.make_async_remote_copy(
            block, block, kvp_ss.at[zz], kvp_rs.at[zz], device_id=(g, partner), device_id_type=MESH
        )

    def pair_stage(kk):
        @pl.loop(0, line)
        def _(i):
            dest = jnp.where(low, line - 1 - i, i)
            pair_out[kk, dest] = product(kk, dest, 1 - c).astype(jnp.bfloat16)
            pair_copy(kk, dest).start()

    def gathered(kk, dest):
        total[...] = product(kk, dest, c)
        pair_copy(kk, dest).wait_recv()
        total[...] += pair_in[kk, dest].astype(jnp.float32)

    def up_stage(kk):
        @pl.loop(0, line - 1 - z)
        def _(d):
            dest = line - 1 - d
            gathered(kk, dest)

            @pl.when(z > 0)
            def _():
                up_copy(kk, dest).wait_recv()
                total[...] += up_in[kk, dest].astype(jnp.float32)

            pair_in[kk, dest] = total[...].astype(jnp.bfloat16)
            up_copy(kk, dest).start()

    def dn_stage(kk):
        @pl.loop(0, z)
        def _(dest):
            gathered(kk, dest)

            @pl.when(z < line - 1)
            def _():
                dn_copy(kk, dest).wait_recv()
                total[...] += dn_in[kk, dest].astype(jnp.float32)

            pair_in[kk, dest] = total[...].astype(jnp.bfloat16)
            dn_copy(kk, dest).start()

    def wait_up_sends(kk):
        @pl.loop(0, line - 1 - z)
        def _(d):
            up_copy(kk, line - 1 - d).wait_send()

    def wait_dn_sends(kk):
        @pl.loop(0, z)
        def _(dest):
            dn_copy(kk, dest).wait_send()

    def rope(x):
        return x * cos_ref[...] + pltpu.roll(x, HEAD_DIM // 2, 1) * sin_ref[...]

    def finish(kk):
        gathered(kk, z)

        @pl.when(z > 0)
        def _():
            up_copy(kk, z).wait_recv()
            total[...] += up_in[kk, z].astype(jnp.float32)

        @pl.when(z < line - 1)
        def _():
            dn_copy(kk, z).wait_recv()
            total[...] += dn_in[kk, z].astype(jnp.float32)

        total[...] += bias_ref[:, pl.ds(offset(kk), width)]

        @pl.when(kk == 0)
        def _():
            kv_ref[s, :, :HEAD_DIM] = rope(total[:, :HEAD_DIM]).astype(jnp.bfloat16)
            kv_ref[s, :, HEAD_DIM:] = total[:, HEAD_DIM:].astype(jnp.bfloat16)
            kv_pair(z).start()

            @pl.when(z < line - 1)
            def _():
                kv_line(z).start()

        @pl.when(kk > 0)
        def _():
            for half in range(width // HEAD_DIM):
                lanes = slice(half * HEAD_DIM, (half + 1) * HEAD_DIM)
                q_ref[:, pl.ds(offset(kk) + half * HEAD_DIM, HEAD_DIM)] = rope(total[:, lanes]).astype(jnp.bfloat16)

    def relay(h):
        @pl.when(h <= z)
        def _():
            zz = z - h
            kv_line(zz).wait_recv()

            @pl.when(z < line - 1)
            def _():
                kv_line(zz).start()

            kv_pair(zz).start()

    pair_stage(0)
    for i in range(1, n):
        id_copy(i).start()

    @pl.loop(0, chunks + 2)
    def _(kk):
        @pl.when(kk >= 2)
        def _():
            @pl.when(low)
            def _():
                wait_up_sends(kk - 2)

            @pl.when(jnp.logical_not(low))
            def _():
                wait_dn_sends(kk - 2)

        @pl.when(kk < chunks)
        def _():
            @pl.when(low)
            def _():
                up_stage(kk)

            @pl.when(jnp.logical_not(low))
            def _():
                dn_stage(kk)

        @pl.when(kk + 1 < chunks)
        def _():
            pair_stage(kk + 1)

        @pl.when((kk >= 1) & (kk <= chunks))
        def _():
            @pl.when(low)
            def _():
                dn_stage(kk - 1)

            @pl.when(jnp.logical_not(low))
            def _():
                up_stage(kk - 1)

        @pl.when(kk >= 2)
        def _():
            finish(kk - 2)

        @pl.when(kk >= 4)
        def _():
            relay(kk - 3)

    @pl.loop(chunks - 1, line)
    def _(h):
        relay(h)

    @pl.loop(0, chunks)
    def _(kk):
        @pl.when(low)
        def _():
            wait_dn_sends(kk)

        @pl.when(jnp.logical_not(low))
        def _():
            wait_up_sends(kk)

        @pl.loop(0, line)
        def _(dest):
            pair_copy(kk, dest).wait_send()

    @pl.loop(0, z + 1)
    def _(zz):
        kv_pair_wait(zz).wait_recv()
        kv_pair(zz).wait_send()

        @pl.when(z < line - 1)
        def _():
            kv_line(zz).wait_send()

    for i in range(1, n):
        id_copy(i).wait_send()
        id_wait(i).wait_recv()


def attention_kernel(blocks, rows, place_ref, q_ref, kv_ref, idall_ref, idcol_ref, out_ref):
    first, last = place_ref[0], place_ref[1]
    scale = HEAD_DIM ** (-0.5)
    row_ids = idcol_ref[:, :1]
    ahead = lax.broadcasted_iota(jnp.int32, (rows, rows), 1) - lax.broadcasted_iota(jnp.int32, (rows, rows), 0)
    ones = jnp.ones((rows, HEAD_DIM), jnp.bfloat16)

    @pl.loop(0, GQA // 2)
    def _(pair):
        lanes = [pl.multiple_of((2 * pair + i) * HEAD_DIM, HEAD_DIM) for i in range(2)]
        queries = [q_ref[:, pl.ds(lane, HEAD_DIM)] for lane in lanes]

        def step(j, state):
            keys = kv_ref[j, :, :HEAD_DIM]
            values = jnp.concatenate([kv_ref[j, :, HEAD_DIM:], ones], axis=1)
            allowed = (row_ids == idall_ref[j, :1, :]) & (ahead <= (last - j) * rows)
            new = []
            for i in range(2):
                row_max, weighted = state[i]
                scores = lax.dot_general(
                    queries[i], keys, (((1,), (1,)), ((), ())), preferred_element_type=jnp.float32
                )
                scores = jnp.where(allowed, scores * scale, neg_large)
                new_max = jnp.maximum(row_max, jnp.max(scores, axis=1, keepdims=True))
                weights = jnp.where(allowed, jnp.exp(scores - new_max), 0.0)
                update = jnp.dot(weights.astype(jnp.bfloat16), values, preferred_element_type=jnp.float32)
                new.append((new_max, weighted * jnp.exp(row_max - new_max) + update))
            return tuple(new)

        initial = (
            jnp.full((rows, 1), neg_large, jnp.float32),
            jnp.zeros((rows, 2 * HEAD_DIM), jnp.float32),
        )
        state = lax.fori_loop(first, last + 1, step, (initial, initial))
        for i in range(2):
            weighted = state[i][1]
            out_ref[:, pl.ds(lanes[i], HEAD_DIM)] = (weighted[:, :HEAD_DIM] / weighted[:, HEAD_DIM:]).astype(
                jnp.bfloat16
            )


def out_kernel(
    groups, tiles, rows, width,
    att_ref, w_ref, out_ref,
    weights, kept, passing_x, passing_y, send1, recv1, send2, recv2,
    w_sem, ss1, rs1, ss2, rs2,
):
    g = lax.axis_index("grp")
    s = lax.axis_index("seq")
    peer_x = g + 1 - 2 * lax.rem(g, 2)
    peer_y = lax.rem(g + 2, groups)
    diagonal = groups - 1 - g
    peers = (peer_x, peer_y)
    half = rows // 2
    order = (diagonal, peer_x, peer_y, g)

    def w_copy(i, t):
        column = pl.multiple_of((order[i] * tiles + t) * width, width)
        return pltpu.make_async_copy(w_ref.at[:, pl.ds(column, width)], weights.at[i, t], w_sem.at[i, t])

    for i in range(4):
        @pl.loop(0, tiles)
        def _(t):
            w_copy(i, t).start()

    barrier = pltpu.get_barrier_semaphore()
    for peer in peers:
        pl.semaphore_signal(barrier, inc=1, device_id=(peer, s), device_id_type=MESH)
    pl.semaphore_wait(barrier, 2)

    def copy1(way, slot, t):
        return pltpu.make_async_remote_copy(
            send1.at[way, slot, t], recv1.at[way, slot, t], ss1.at[way, slot, t], rs1.at[way, slot, t],
            device_id=(peers[way], s), device_id_type=MESH,
        )

    def copy2(way, t):
        return pltpu.make_async_remote_copy(
            send2.at[way, t], recv2.at[way, t], ss2.at[way, t], rs2.at[way, t],
            device_id=(peers[way], s), device_id_type=MESH,
        )

    def product(i, t):
        w_copy(i, t).wait()
        return jnp.dot(att_ref[...], weights[i, t], preferred_element_type=jnp.float32)

    @pl.loop(0, tiles)
    def _(t):
        value = product(0, t).astype(jnp.bfloat16)
        send1[0, 0, t] = value[:half]
        send1[1, 0, t] = value[half:]
        copy1(0, 0, t).start()
        copy1(1, 0, t).start()

    @pl.loop(0, tiles)
    def _(t):
        value = product(1, t)
        send1[0, 1, t] = value[:half].astype(jnp.bfloat16)
        copy1(0, 1, t).start()
        passing_x[t] = value[half:]
        value = product(2, t)
        send1[1, 1, t] = value[half:].astype(jnp.bfloat16)
        copy1(1, 1, t).start()
        passing_y[t] = value[:half]

    @pl.loop(0, tiles)
    def _(t):
        copy1(1, 0, t).wait_recv()
        send2[0, t] = (passing_x[t] + recv1[1, 0, t].astype(jnp.float32)).astype(jnp.bfloat16)
        copy2(0, t).start()
        copy1(0, 0, t).wait_recv()
        send2[1, t] = (passing_y[t] + recv1[0, 0, t].astype(jnp.float32)).astype(jnp.bfloat16)
        copy2(1, t).start()

    @pl.loop(0, tiles)
    def _(t):
        kept[t] = product(3, t)

    for t in range(tiles):
        copy1(0, 1, t).wait_recv()
        copy1(1, 1, t).wait_recv()
        copy2(0, t).wait_recv()
        copy2(1, t).wait_recv()
        lanes = slice(t * width, (t + 1) * width)
        out_ref[:half, lanes] = (
            kept[t, :half] + recv1[0, 1, t].astype(jnp.float32) + recv2[1, t].astype(jnp.float32)
        ).astype(jnp.bfloat16)
        out_ref[half:, lanes] = (
            kept[t, half:] + recv1[1, 1, t].astype(jnp.float32) + recv2[0, t].astype(jnp.float32)
        ).astype(jnp.bfloat16)

    @pl.loop(0, tiles)
    def _(t):
        for way in range(2):
            copy1(way, 0, t).wait_send()
            copy1(way, 1, t).wait_send()
            copy2(way, t).wait_send()


def body(seq, groups, tokens, proj_weight, proj_bias, out_weight, doc_ids):
    rows = doc_ids.shape[0]
    columns = proj_weight.shape[1]
    width = 2 * HEAD_DIM
    chunks = columns // width
    line = seq // 2
    q_width = GQA * HEAD_DIM
    start = lax.axis_index("seq") * rows
    positions = start + jnp.arange(rows, dtype=jnp.int32)
    cosine, sine = rope_tables(positions, HEAD_DIM)
    vmem = pl.BlockSpec(memory_space=pltpu.VMEM)
    dma = pltpu.SemaphoreType.DMA
    bf16, f32 = jnp.bfloat16, jnp.float32
    limit = 62 * 1024 * 1024

    queries, kv, id_blocks = pl.pallas_call(
        functools.partial(proj_kernel, line, chunks, rows, width),
        out_shape=(
            jax.ShapeDtypeStruct((rows, q_width), bf16),
            jax.ShapeDtypeStruct((seq, rows, width), bf16),
            jax.ShapeDtypeStruct((seq, 8, rows), jnp.int32),
        ),
        in_specs=[vmem] * 6,
        out_specs=(vmem, vmem, vmem),
        scratch_shapes=[pltpu.VMEM((chunks, line, rows, width), bf16)] * 4
        + [pltpu.VMEM((rows, width), f32)]
        + [dma((chunks, line))] * 5
        + [dma((seq,))] * 2
        + [dma((line,))] * 4,
        compiler_params=pltpu.CompilerParams(collective_id=0, has_side_effects=True, vmem_limit_bytes=limit),
        name="proj_scatter",
    )(
        tokens,
        proj_weight,
        proj_bias.astype(f32)[None, :],
        cosine,
        sine,
        jnp.broadcast_to(doc_ids[None, :], (8, rows)),
    )

    place = jnp.stack(
        [jnp.sum((id_blocks[:, 0, rows - 1] < doc_ids[0]).astype(jnp.int32)), lax.axis_index("seq")]
    ).astype(jnp.int32)
    attended = pl.pallas_call(
        functools.partial(attention_kernel, seq, rows),
        out_shape=jax.ShapeDtypeStruct((rows, q_width), bf16),
        in_specs=[pl.BlockSpec(memory_space=pltpu.SMEM)] + [vmem] * 4,
        out_specs=vmem,
        compiler_params=pltpu.CompilerParams(vmem_limit_bytes=limit),
        name="attention",
    )(place, queries, kv, id_blocks, jnp.broadcast_to(doc_ids[:, None], (rows, HEAD_DIM)))

    block = out_weight.shape[1] // groups
    tile = 2 * width
    tiles = block // tile
    half = rows // 2
    return pl.pallas_call(
        functools.partial(out_kernel, groups, tiles, rows, tile),
        out_shape=jax.ShapeDtypeStruct((rows, block), bf16),
        in_specs=[vmem, pl.BlockSpec(memory_space=pl.ANY)],
        out_specs=vmem,
        scratch_shapes=[
            pltpu.VMEM((4, tiles, q_width, tile), bf16),
            pltpu.VMEM((tiles, rows, tile), f32),
            pltpu.VMEM((tiles, half, tile), f32),
            pltpu.VMEM((tiles, half, tile), f32),
            pltpu.VMEM((2, 2, tiles, half, tile), bf16),
            pltpu.VMEM((2, 2, tiles, half, tile), bf16),
            pltpu.VMEM((2, tiles, half, tile), bf16),
            pltpu.VMEM((2, tiles, half, tile), bf16),
            dma((4, tiles)),
            dma((2, 2, tiles)),
            dma((2, 2, tiles)),
            dma((2, tiles)),
            dma((2, tiles)),
        ],
        compiler_params=pltpu.CompilerParams(collective_id=1, has_side_effects=True, vmem_limit_bytes=limit),
        name="out_scatter",
    )(attended, out_weight)


def solution(mesh):
    return jax.shard_map(
        functools.partial(body, mesh.shape["seq"], mesh.shape["grp"]),
        mesh=mesh,
        in_specs=(P(None, "seq"), P("seq", "grp"), P("grp"), P("grp", None), P("seq")),
        out_specs=P("seq", "grp"),
        check_vma=False,
    )
```

```python
import functools

import jax
import jax.numpy as jnp
from jax import lax
from jax.experimental import pallas as pl
from jax.experimental.pallas import tpu as pltpu
from jax.sharding import PartitionSpec as P

HEAD_DIM = 128
GQA = 8
MESH = pl.DeviceIdType.MESH

theta_base = 1000000.0
neg_large = -1e30


def layer_kernel(
    line, chunks, rows, width, groups, tiles, wide, slots,
    tok_ref, w_ref, bias_ref, freq_ref, ids_ref, ow_ref,
    out_ref,
    pair_out, pair_in, up_in, dn_in, total, queries, kv_ref, attended, ids_own, ids_col, idall_ref,
    bias, cos_ref, sin_ref, weights, kept, send1, recv1, send2, recv2,
    pair_ss, pair_rs, line_ss, up_rs, dn_rs, id_ss, id_rs, kvl_ss, kvl_rs, kvp_ss, kvp_rs,
    w_sem, ss1, rs1, ss2, rs2,
):
    g = lax.axis_index("grp")
    s = lax.axis_index("seq")
    z, c = s // 2, lax.rem(s, 2)
    n = 2 * line
    partner = s + 1 - 2 * c
    low = z < line // 2
    half = rows // 2
    peer_x = g + 1 - 2 * lax.rem(g, 2)
    peer_y = lax.rem(g + 2, groups)
    passes = 4 * tiles

    def first_peer(t):
        return jnp.where(lax.rem(t, 2) == 0, peer_x, peer_y)

    def second_peer(t):
        return jnp.where(lax.rem(t, 2) == 0, peer_y, peer_x)

    def w_copy(m):
        pos, t = lax.rem(m // tiles, 4), lax.rem(m, tiles)
        block = jnp.where(
            pos == 0, groups - 1 - g, jnp.where(pos == 1, first_peer(t), jnp.where(pos == 2, g, second_peer(t)))
        )
        column = pl.multiple_of((block * tiles + t) * wide, wide)
        slot = lax.rem(m, slots)
        return pltpu.make_async_copy(ow_ref.at[:, pl.ds(column, wide)], weights.at[slot], w_sem.at[slot])

    @pl.loop(0, slots)
    def _(m):
        w_copy(m).start()

    row_ids = jnp.broadcast_to(ids_ref[...].reshape(1, rows), (HEAD_DIM, rows))
    ids_own[...] = row_ids[:8]
    ids_col[...] = row_ids.T
    bias[...] = jnp.broadcast_to(bias_ref[...].astype(jnp.float32), bias.shape)

    barrier = pltpu.get_barrier_semaphore()
    for i in range(1, n):
        pl.semaphore_signal(barrier, inc=1, device_id=(g, lax.rem(s + i, n)), device_id_type=MESH)
    for peer in (peer_x, peer_y):
        pl.semaphore_signal(barrier, inc=1, device_id=(peer, s), device_id_type=MESH)
    pl.semaphore_wait(barrier, n + 1)

    def id_copy(i):
        return pltpu.make_async_remote_copy(
            ids_own, idall_ref.at[s], id_ss.at[i], id_rs.at[i],
            device_id=(g, lax.rem(s + i, n)), device_id_type=MESH,
        )

    def id_wait(i):
        return pltpu.make_async_remote_copy(
            ids_own, idall_ref.at[lax.rem(s + n - i, n)], id_ss.at[i], id_rs.at[i],
            device_id=(g, lax.rem(s + i, n)), device_id_type=MESH,
        )

    idall_ref[s] = ids_own[...]

    def product(kk, dest, core, put):
        row = (2 * dest + core) * rows

        @pl.when(kk == 0)
        def _():
            put(slice(None), jnp.dot(
                tok_ref[pl.ds(pl.multiple_of(row, rows), rows), :], w_ref[:, (chunks - 1) * width :],
                preferred_element_type=jnp.float32,
            ))

        @pl.when(kk > 0)
        def _():
            part = pl.multiple_of(row + (kk - 1) // 2 * half, half)
            column = pl.multiple_of(lax.rem(kk - 1, 2) * 2 * width, 2 * width)
            value = jnp.dot(
                tok_ref[pl.ds(part, half), :], w_ref[:, pl.ds(column, 2 * width)],
                preferred_element_type=jnp.float32,
            )
            put(slice(0, half), value[:, :width])
            put(slice(half, rows), value[:, width:])

    def pair_copy(kk, dest):
        return pltpu.make_async_remote_copy(
            pair_out.at[lax.rem(kk, 2), dest], pair_in.at[kk, dest], pair_ss.at[kk, dest], pair_rs.at[kk, dest],
            device_id=(g, partner), device_id_type=MESH,
        )

    def up_copy(kk, dest):
        return pltpu.make_async_remote_copy(
            pair_in.at[kk, dest], up_in.at[kk, dest], line_ss.at[kk, dest], up_rs.at[kk, dest],
            device_id=(g, lax.rem(s + 2, n)), device_id_type=MESH,
        )

    def dn_copy(kk, dest):
        return pltpu.make_async_remote_copy(
            pair_in.at[kk, dest], dn_in.at[kk, dest], line_ss.at[kk, dest], dn_rs.at[kk, dest],
            device_id=(g, lax.rem(s + n - 2, n)), device_id_type=MESH,
        )

    def kv_line(zz):
        block = kv_ref.at[2 * zz + c]
        return pltpu.make_async_remote_copy(
            block, block, kvl_ss.at[zz], kvl_rs.at[zz], device_id=(g, lax.rem(s + 2, n)), device_id_type=MESH
        )

    def kv_pair(zz):
        block = kv_ref.at[2 * zz + c]
        return pltpu.make_async_remote_copy(
            block, block, kvp_ss.at[zz], kvp_rs.at[zz], device_id=(g, partner), device_id_type=MESH
        )

    def kv_pair_wait(zz):
        block = kv_ref.at[2 * zz + 1 - c]
        return pltpu.make_async_remote_copy(
            block, block, kvp_ss.at[zz], kvp_rs.at[zz], device_id=(g, partner), device_id_type=MESH
        )

    def pair_stage(kk):
        @pl.loop(0, line)
        def _(i):
            dest = jnp.where(low, line - 1 - i, i)

            @pl.when(kk >= 2)
            def _():
                pair_copy(kk - 2, dest).wait_send()

            def put(part, value):
                pair_out[lax.rem(kk, 2), dest, part] = value.astype(jnp.bfloat16)

            product(kk, dest, 1 - c, put)
            pair_copy(kk, dest).start()

    def gathered(kk, dest):
        def put(part, value):
            total[part] = value

        product(kk, dest, c, put)
        pair_copy(kk, dest).wait_recv()
        total[...] += pair_in[kk, dest].astype(jnp.float32)

    def up_stage(kk):
        @pl.loop(0, line - 1 - z)
        def _(d):
            dest = line - 1 - d
            gathered(kk, dest)

            @pl.when(z > 0)
            def _():
                up_copy(kk, dest).wait_recv()
                total[...] += up_in[kk, dest].astype(jnp.float32)

            pair_in[kk, dest] = total[...].astype(jnp.bfloat16)
            up_copy(kk, dest).start()

    def dn_stage(kk):
        @pl.loop(0, z)
        def _(dest):
            gathered(kk, dest)

            @pl.when(z < line - 1)
            def _():
                dn_copy(kk, dest).wait_recv()
                total[...] += dn_in[kk, dest].astype(jnp.float32)

            pair_in[kk, dest] = total[...].astype(jnp.bfloat16)
            dn_copy(kk, dest).start()

    def wait_up_sends(kk):
        @pl.loop(0, line - 1 - z)
        def _(d):
            up_copy(kk, line - 1 - d).wait_send()

    def wait_dn_sends(kk):
        @pl.loop(0, z)
        def _(dest):
            dn_copy(kk, dest).wait_send()

    def rope(x, cosine, sine):
        return x * cosine + pltpu.roll(x, HEAD_DIM // 2, 1) * sine

    def finish(kk):
        gathered(kk, z)

        @pl.when(z > 0)
        def _():
            up_copy(kk, z).wait_recv()
            total[...] += up_in[kk, z].astype(jnp.float32)

        @pl.when(z < line - 1)
        def _():
            dn_copy(kk, z).wait_recv()
            total[...] += dn_in[kk, z].astype(jnp.float32)

        @pl.when(kk == 0)
        def _():
            value = total[...] + bias[:1, (chunks - 1) * width :]
            kv_ref[s, :, :HEAD_DIM] = rope(value[:, :HEAD_DIM], cos_ref[...], sin_ref[...]).astype(jnp.bfloat16)
            kv_ref[s, :, HEAD_DIM:] = value[:, HEAD_DIM:].astype(jnp.bfloat16)
            kv_pair(z).start()

            @pl.when(z < line - 1)
            def _():
                kv_line(z).start()

        @pl.when(kk > 0)
        def _():
            side = (kk - 1) // 2
            group = lax.rem(kk - 1, 2)
            mine = pl.ds(pl.multiple_of(side * half, half), half)
            for i in range(4):
                head = group * 4 + i
                lane = pl.multiple_of(head * HEAD_DIM, HEAD_DIM)
                value = total[(i // 2) * half : (i // 2 + 1) * half, (i % 2) * HEAD_DIM : (i % 2 + 1) * HEAD_DIM]
                value = rope(value + bias[:1, pl.ds(lane, HEAD_DIM)], cos_ref[mine, :], sin_ref[mine, :])
                queries[side, pl.ds(pl.multiple_of(head * half, half), half), :] = value.astype(jnp.bfloat16)

    def relay(h):
        @pl.when(h <= z)
        def _():
            zz = z - h
            kv_line(zz).wait_recv()

            @pl.when(z < line - 1)
            def _():
                kv_line(zz).start()

            kv_pair(zz).start()

    def attend(side):
        ahead = lax.broadcasted_iota(jnp.int32, (half, rows), 1) - lax.broadcasted_iota(jnp.int32, (half, rows), 0)
        ahead = ahead - side * half
        mine_ids = ids_col[pl.ds(pl.multiple_of(side * half, half), half), :1]
        ones = jnp.ones((rows, HEAD_DIM), jnp.bfloat16)
        scale = HEAD_DIM ** (-0.5)

        @pl.loop(0, GQA // 4)
        def _(quad):
            tops = [pl.multiple_of((2 * quad + i) * 2 * half, 2 * half) for i in range(2)]
            stacked = [queries[side, pl.ds(top, 2 * half), :] for top in tops]

            def step(j, state):
                keys = kv_ref[j, :, :HEAD_DIM]
                values = jnp.concatenate([kv_ref[j, :, HEAD_DIM:], ones], axis=1)
                allowed = (mine_ids == idall_ref[j, :1, :]) & (ahead <= (s - j) * rows)
                allowed = jnp.concatenate([allowed, allowed], axis=0)
                new = []
                for i in range(2):
                    row_max, weighted = state[i]
                    scores = lax.dot_general(
                        stacked[i], keys, (((1,), (1,)), ((), ())), preferred_element_type=jnp.float32
                    )
                    scores = jnp.where(allowed, scores * scale, neg_large)
                    new_max = jnp.maximum(row_max, jnp.max(scores, axis=1, keepdims=True))
                    exps = jnp.where(allowed, jnp.exp(scores - new_max), 0.0)
                    update = jnp.dot(exps.astype(jnp.bfloat16), values, preferred_element_type=jnp.float32)
                    new.append((new_max, weighted * jnp.exp(row_max - new_max) + update))
                return tuple(new)

            initial = (
                jnp.full((2 * half, 1), neg_large, jnp.float32),
                jnp.zeros((2 * half, 2 * HEAD_DIM), jnp.float32),
            )
            state = lax.fori_loop(0, s + 1, step, (initial, initial))
            for i in range(2):
                weighted = state[i][1]
                value = (weighted[:, :HEAD_DIM] / weighted[:, HEAD_DIM:]).astype(jnp.bfloat16)
                for part in range(2):
                    lane = pl.multiple_of((4 * quad + 2 * i + part) * HEAD_DIM, HEAD_DIM)
                    attended[side, :, pl.ds(lane, HEAD_DIM)] = value[part * half : (part + 1) * half]

    def mixed(side, pos, t):
        m = side * passes + pos * tiles + t
        w_copy(m).wait()
        value = jnp.dot(attended[side], weights[lax.rem(m, slots)], preferred_element_type=jnp.float32)

        @pl.when(m + slots < 2 * passes)
        def _():
            w_copy(m + slots).start()

        return value

    def copy1(side, slot, t):
        return pltpu.make_async_remote_copy(
            send1.at[side, slot, t], recv1.at[side, slot, t], ss1.at[side, slot, t], rs1.at[side, slot, t],
            device_id=(first_peer(t), s), device_id_type=MESH,
        )

    def copy2(side, t):
        return pltpu.make_async_remote_copy(
            send2.at[side, t], recv2.at[side, t], ss2.at[side, t], rs2.at[side, t],
            device_id=(second_peer(t), s), device_id_type=MESH,
        )

    def send_out(side):
        @pl.loop(0, 2 * tiles)
        def _(m):
            slot, t = m // tiles, lax.rem(m, tiles)
            send1[side, slot, t] = mixed(side, slot, t).astype(jnp.bfloat16)
            copy1(side, slot, t).start()

    def pass_on(side):
        @pl.loop(0, tiles)
        def _(t):
            kept[side, t] = mixed(side, 2, t)

        @pl.loop(0, tiles)
        def _(t):
            value = mixed(side, 3, t)
            copy1(side, 0, t).wait_recv()
            send2[side, t] = (value + recv1[side, 0, t].astype(jnp.float32)).astype(jnp.bfloat16)
            copy2(side, t).start()

    def collect(side):
        @pl.loop(0, tiles)
        def _(t):
            copy1(side, 1, t).wait_recv()
            copy2(side, t).wait_recv()
            value = kept[side, t] + recv1[side, 1, t].astype(jnp.float32) + recv2[side, t].astype(jnp.float32)
            mine = pl.ds(pl.multiple_of(side * half, half), half)
            out_ref[mine, pl.ds(pl.multiple_of(t * wide, wide), wide)] = value.astype(jnp.bfloat16)

    def primary(kk):
        @pl.when(low)
        def _():
            up_stage(kk)

        @pl.when(jnp.logical_not(low))
        def _():
            dn_stage(kk)

    def secondary(kk):
        @pl.when(low)
        def _():
            dn_stage(kk)

        @pl.when(jnp.logical_not(low))
        def _():
            up_stage(kk)

    def wait_primary(kk):
        @pl.when(low)
        def _():
            wait_up_sends(kk)

        @pl.when(jnp.logical_not(low))
        def _():
            wait_dn_sends(kk)

    def wait_secondary(kk):
        @pl.when(low)
        def _():
            wait_dn_sends(kk)

        @pl.when(jnp.logical_not(low))
        def _():
            wait_up_sends(kk)

    pair_stage(0)
    for i in range(1, n):
        id_copy(i).start()

    @pl.loop(0, chunks)
    def _(kk):
        @pl.when(kk >= 2)
        def _():
            wait_primary(kk - 2)

        primary(kk)

        @pl.when(kk == 0)
        def _():
            angles = (s * rows + lax.broadcasted_iota(jnp.int32, (rows, HEAD_DIM), 0)).astype(
                jnp.float32
            ) * freq_ref[...]
            lane = lax.broadcasted_iota(jnp.int32, (rows, HEAD_DIM), 1)
            sine = jnp.sin(angles)
            cos_ref[...] = jnp.cos(angles)
            sin_ref[...] = jnp.where(lane < HEAD_DIM // 2, -sine, sine)

        @pl.when(kk + 1 < chunks)
        def _():
            pair_stage(kk + 1)

        @pl.when(kk >= 1)
        def _():
            secondary(kk - 1)

        @pl.when(kk >= 2)
        def _():
            finish(kk - 2)

    for i in range(1, n):
        id_copy(i).wait_send()
        id_wait(i).wait_recv()

    @pl.loop(1, line)
    def _(h):
        relay(h)

    @pl.loop(0, z + 1)
    def _(zz):
        kv_pair_wait(zz).wait_recv()

    @pl.loop(0, 2)
    def _(side):
        attend(side)
        send_out(side)

        @pl.when(side == 0)
        def _():
            secondary(chunks - 1)
            finish(chunks - 2)

        pass_on(side)

        @pl.when(side == 0)
        def _():
            finish(chunks - 1)

    @pl.loop(0, 2)
    def _(side):
        collect(side)

    @pl.loop(0, chunks)
    def _(kk):
        @pl.when(kk >= chunks - 2)
        def _():
            wait_primary(kk)

            @pl.loop(0, line)
            def _(dest):
                pair_copy(kk, dest).wait_send()

        wait_secondary(kk)

    @pl.loop(0, z + 1)
    def _(zz):
        kv_pair(zz).wait_send()

        @pl.when(z < line - 1)
        def _():
            kv_line(zz).wait_send()

    @pl.loop(0, 2)
    def _(side):
        @pl.loop(0, tiles)
        def _(t):
            copy1(side, 0, t).wait_send()
            copy1(side, 1, t).wait_send()
            copy2(side, t).wait_send()


def body(seq, groups, tokens, proj_weight, proj_bias, out_weight, doc_ids):
    rows = doc_ids.shape[0]
    columns = proj_weight.shape[1]
    width = 2 * HEAD_DIM
    chunks = columns // width
    line = seq // 2
    half = rows // 2
    q_width = GQA * HEAD_DIM
    block = out_weight.shape[1] // groups
    wide = 4 * HEAD_DIM
    tiles = block // wide
    slots = 2 * tiles
    inverse_freq = theta_base ** (-(jnp.arange(HEAD_DIM // 2, dtype=jnp.float32) * 2.0) / HEAD_DIM)
    freq = jnp.concatenate([inverse_freq, inverse_freq])[None, :]
    vmem = pl.BlockSpec(memory_space=pltpu.VMEM)
    dma = pltpu.SemaphoreType.DMA
    bf16, f32, i32 = jnp.bfloat16, jnp.float32, jnp.int32

    return pl.pallas_call(
        functools.partial(layer_kernel, line, chunks, rows, width, groups, tiles, wide, slots),
        out_shape=jax.ShapeDtypeStruct((rows, block), bf16),
        in_specs=[vmem] * 5 + [pl.BlockSpec(memory_space=pl.ANY)],
        out_specs=vmem,
        scratch_shapes=[
            pltpu.VMEM((2, line, rows, width), bf16),
            pltpu.VMEM((chunks, line, rows, width), bf16),
            pltpu.VMEM((chunks, line, rows, width), bf16),
            pltpu.VMEM((chunks, line, rows, width), bf16),
            pltpu.VMEM((rows, width), f32),
            pltpu.VMEM((2, GQA * half, HEAD_DIM), bf16),
            pltpu.VMEM((seq, rows, width), bf16),
            pltpu.VMEM((2, half, q_width), bf16),
            pltpu.VMEM((8, rows), i32),
            pltpu.VMEM((rows, HEAD_DIM), i32),
            pltpu.VMEM((seq, 8, rows), i32),
            pltpu.VMEM((8, columns), f32),
            pltpu.VMEM((rows, HEAD_DIM), f32),
            pltpu.VMEM((rows, HEAD_DIM), f32),
            pltpu.VMEM((slots, q_width, wide), bf16),
            pltpu.VMEM((2, tiles, half, wide), f32),
            pltpu.VMEM((2, 2, tiles, half, wide), bf16),
            pltpu.VMEM((2, 2, tiles, half, wide), bf16),
            pltpu.VMEM((2, tiles, half, wide), bf16),
            pltpu.VMEM((2, tiles, half, wide), bf16),
        ]
        + [dma((chunks, line))] * 5
        + [dma((seq,))] * 2
        + [dma((line,))] * 4
        + [dma((slots,)), dma((2, 2, tiles)), dma((2, 2, tiles)), dma((2, tiles)), dma((2, tiles))],
        compiler_params=pltpu.CompilerParams(
            collective_id=0, has_side_effects=True, vmem_limit_bytes=67043328
        ),
        name="layer",
    )(tokens, proj_weight, proj_bias[None, :], freq, doc_ids[None, :], out_weight)


def solution(mesh):
    return jax.shard_map(
        functools.partial(body, mesh.shape["seq"], mesh.shape["grp"]),
        mesh=mesh,
        in_specs=(P(None, "seq"), P("seq", "grp"), P("grp"), P("grp", None), P("seq")),
        out_specs=P("seq", "grp"),
        check_vma=False,
    )
```

```python
import functools

import jax
import jax.numpy as jnp
from jax import lax
from jax.experimental import pallas as pl
from jax.experimental.pallas import tpu as pltpu
from jax.sharding import PartitionSpec as P

HEAD_DIM = 128
GQA = 8
MESH = pl.DeviceIdType.MESH

theta_base = 1000000.0
neg_large = -1e30
log2_e = 1.4426950408889634


def layer_kernel(
    line, chunks, rows, width, groups, tiles, wide, slots,
    tok_ref, w_ref, bias_ref, freq_ref, ids_ref, ow_ref,
    out_ref,
    pair_out, pair_in, up_in, dn_in, total, queries, kv_ref, attended, ids_own, ids_col, idall_ref,
    bias, cos_ref, sin_ref, weights, kept, send1, recv1, send2, recv2,
    pair_ss, pair_rs, line_ss, up_rs, dn_rs, id_ss, id_rs, kvl_ss, kvl_rs, kvp_ss, kvp_rs,
    w_sem, ss1, rs1, ss2, rs2,
):
    g = lax.axis_index("grp")
    s = lax.axis_index("seq")
    z, c = s // 2, lax.rem(s, 2)
    n = 2 * line
    partner = s + 1 - 2 * c
    low = z < line // 2
    half = rows // 2
    peer_x = g + 1 - 2 * lax.rem(g, 2)
    peer_y = lax.rem(g + 2, groups)
    passes = 4 * tiles

    def first_peer(t):
        return jnp.where(lax.rem(t, 2) == 0, peer_x, peer_y)

    def second_peer(t):
        return jnp.where(lax.rem(t, 2) == 0, peer_y, peer_x)

    def w_copy(m):
        pos, t = lax.rem(m // tiles, 4), lax.rem(m, tiles)
        block = jnp.where(
            pos == 0, groups - 1 - g, jnp.where(pos == 1, first_peer(t), jnp.where(pos == 2, g, second_peer(t)))
        )
        column = pl.multiple_of((block * tiles + t) * wide, wide)
        slot = lax.rem(m, slots)
        return pltpu.make_async_copy(ow_ref.at[:, pl.ds(column, wide)], weights.at[slot], w_sem.at[slot])

    @pl.loop(0, slots)
    def _(m):
        w_copy(m).start()

    row_ids = jnp.broadcast_to(ids_ref[...].reshape(1, rows), (HEAD_DIM, rows))
    ids_own[...] = row_ids[:8]
    ids_col[...] = row_ids.T
    bias[...] = jnp.broadcast_to(bias_ref[...].astype(jnp.float32), bias.shape)

    barrier = pltpu.get_barrier_semaphore()
    for i in range(1, n):
        pl.semaphore_signal(barrier, inc=1, device_id=(g, lax.rem(s + i, n)), device_id_type=MESH)
    for peer in (peer_x, peer_y):
        pl.semaphore_signal(barrier, inc=1, device_id=(peer, s), device_id_type=MESH)
    pl.semaphore_wait(barrier, n + 1)

    def id_copy(i):
        return pltpu.make_async_remote_copy(
            ids_own, idall_ref.at[s], id_ss.at[i], id_rs.at[i],
            device_id=(g, lax.rem(s + i, n)), device_id_type=MESH,
        )

    def id_wait(i):
        return pltpu.make_async_remote_copy(
            ids_own, idall_ref.at[lax.rem(s + n - i, n)], id_ss.at[i], id_rs.at[i],
            device_id=(g, lax.rem(s + i, n)), device_id_type=MESH,
        )

    idall_ref[s] = ids_own[...]

    def product(kk, dest, core, put):
        row = (2 * dest + core) * rows

        @pl.when(kk == 0)
        def _():
            put(slice(None), jnp.dot(
                tok_ref[pl.ds(pl.multiple_of(row, rows), rows), :], w_ref[:, (chunks - 1) * width :],
                preferred_element_type=jnp.float32,
            ))

        @pl.when(kk > 0)
        def _():
            part = pl.multiple_of(row + (kk - 1) // 2 * half, half)
            column = pl.multiple_of(lax.rem(kk - 1, 2) * 2 * width, 2 * width)
            value = jnp.dot(
                tok_ref[pl.ds(part, half), :], w_ref[:, pl.ds(column, 2 * width)],
                preferred_element_type=jnp.float32,
            )
            put(slice(0, half), value[:, :width])
            put(slice(half, rows), value[:, width:])

    def pair_copy(kk, dest):
        return pltpu.make_async_remote_copy(
            pair_out.at[lax.rem(kk, 2), dest], pair_in.at[kk, dest], pair_ss.at[kk, dest], pair_rs.at[kk, dest],
            device_id=(g, partner), device_id_type=MESH,
        )

    def up_copy(kk, dest):
        return pltpu.make_async_remote_copy(
            pair_in.at[kk, dest], up_in.at[kk, dest], line_ss.at[kk, dest], up_rs.at[kk, dest],
            device_id=(g, lax.rem(s + 2, n)), device_id_type=MESH,
        )

    def dn_copy(kk, dest):
        return pltpu.make_async_remote_copy(
            pair_in.at[kk, dest], dn_in.at[kk, dest], line_ss.at[kk, dest], dn_rs.at[kk, dest],
            device_id=(g, lax.rem(s + n - 2, n)), device_id_type=MESH,
        )

    def kv_line(zz):
        block = kv_ref.at[2 * zz + c]
        return pltpu.make_async_remote_copy(
            block, block, kvl_ss.at[zz], kvl_rs.at[zz], device_id=(g, lax.rem(s + 2, n)), device_id_type=MESH
        )

    def kv_pair(zz):
        block = kv_ref.at[2 * zz + c]
        return pltpu.make_async_remote_copy(
            block, block, kvp_ss.at[zz], kvp_rs.at[zz], device_id=(g, partner), device_id_type=MESH
        )

    def kv_pair_wait(zz):
        block = kv_ref.at[2 * zz + 1 - c]
        return pltpu.make_async_remote_copy(
            block, block, kvp_ss.at[zz], kvp_rs.at[zz], device_id=(g, partner), device_id_type=MESH
        )

    def pair_stage(kk):
        @pl.loop(0, line)
        def _(i):
            dest = jnp.where(low, line - 1 - i, i)

            @pl.when(kk >= 2)
            def _():
                pair_copy(kk - 2, dest).wait_send()

            def put(part, value):
                pair_out[lax.rem(kk, 2), dest, part] = value.astype(jnp.bfloat16)

            product(kk, dest, 1 - c, put)
            pair_copy(kk, dest).start()

    def gathered(kk, dest):
        def put(part, value):
            total[part] = value

        product(kk, dest, c, put)
        pair_copy(kk, dest).wait_recv()
        total[...] += pair_in[kk, dest].astype(jnp.float32)

    def up_stage(kk):
        @pl.loop(0, line - 1 - z)
        def _(d):
            dest = line - 1 - d
            gathered(kk, dest)

            @pl.when(z > 0)
            def _():
                up_copy(kk, dest).wait_recv()
                total[...] += up_in[kk, dest].astype(jnp.float32)

            pair_in[kk, dest] = total[...].astype(jnp.bfloat16)
            up_copy(kk, dest).start()

    def dn_stage(kk):
        @pl.loop(0, z)
        def _(dest):
            gathered(kk, dest)

            @pl.when(z < line - 1)
            def _():
                dn_copy(kk, dest).wait_recv()
                total[...] += dn_in[kk, dest].astype(jnp.float32)

            pair_in[kk, dest] = total[...].astype(jnp.bfloat16)
            dn_copy(kk, dest).start()

    def wait_up_sends(kk):
        @pl.loop(0, line - 1 - z)
        def _(d):
            up_copy(kk, line - 1 - d).wait_send()

    def wait_dn_sends(kk):
        @pl.loop(0, z)
        def _(dest):
            dn_copy(kk, dest).wait_send()

    def rope(x, cosine, sine):
        return x * cosine + pltpu.roll(x, HEAD_DIM // 2, 1) * sine

    def finish(kk):
        gathered(kk, z)

        @pl.when(z > 0)
        def _():
            up_copy(kk, z).wait_recv()
            total[...] += up_in[kk, z].astype(jnp.float32)

        @pl.when(z < line - 1)
        def _():
            dn_copy(kk, z).wait_recv()
            total[...] += dn_in[kk, z].astype(jnp.float32)

        @pl.when(kk == 0)
        def _():
            value = total[...] + bias[:1, (chunks - 1) * width :]
            kv_ref[s, :, :HEAD_DIM] = rope(value[:, :HEAD_DIM], cos_ref[...], sin_ref[...]).astype(jnp.bfloat16)
            kv_ref[s, :, HEAD_DIM:] = value[:, HEAD_DIM:].astype(jnp.bfloat16)
            kv_pair(z).start()

            @pl.when(z < line - 1)
            def _():
                kv_line(z).start()

        @pl.when(kk > 0)
        def _():
            side = (kk - 1) // 2
            group = lax.rem(kk - 1, 2)
            mine = pl.ds(pl.multiple_of(side * half, half), half)
            for i in range(4):
                head = group * 4 + i
                lane = pl.multiple_of(head * HEAD_DIM, HEAD_DIM)
                value = total[(i // 2) * half : (i // 2 + 1) * half, (i % 2) * HEAD_DIM : (i % 2 + 1) * HEAD_DIM]
                value = rope(value + bias[:1, pl.ds(lane, HEAD_DIM)], cos_ref[mine, :], sin_ref[mine, :])
                queries[side, pl.ds(pl.multiple_of(head * half, half), half), :] = value.astype(jnp.bfloat16)

    def relay(h):
        @pl.when(h <= z)
        def _():
            zz = z - h
            kv_line(zz).wait_recv()

            @pl.when(z < line - 1)
            def _():
                kv_line(zz).start()

            kv_pair(zz).start()

    def attend(side):
        ahead = lax.broadcasted_iota(jnp.int32, (half, rows), 1) - lax.broadcasted_iota(jnp.int32, (half, rows), 0)
        ahead = ahead - side * half
        mine_ids = ids_col[pl.ds(pl.multiple_of(side * half, half), half), :1]
        ones = jnp.ones((rows, HEAD_DIM), jnp.bfloat16)
        scale = HEAD_DIM ** (-0.5) * log2_e

        @pl.loop(0, GQA // 4)
        def _(quad):
            tops = [pl.multiple_of((2 * quad + i) * 2 * half, 2 * half) for i in range(2)]
            stacked = [queries[side, pl.ds(top, 2 * half), :] for top in tops]

            def step(j, state):
                keys = kv_ref[j, :, :HEAD_DIM]
                values = jnp.concatenate([kv_ref[j, :, HEAD_DIM:], ones], axis=1)
                allowed = (mine_ids == idall_ref[j, :1, :]) & (ahead <= (s - j) * rows)
                allowed = jnp.concatenate([allowed, allowed], axis=0)
                new = []
                for i in range(2):
                    row_max, weighted = state[i]
                    scores = lax.dot_general(
                        stacked[i], keys, (((1,), (1,)), ((), ())), preferred_element_type=jnp.float32
                    )
                    scores = jnp.where(allowed, scores * scale, neg_large)
                    new_max = jnp.maximum(row_max, jnp.max(scores, axis=1, keepdims=True))
                    exps = jnp.exp2(scores - new_max)
                    update = jnp.dot(exps.astype(jnp.bfloat16), values, preferred_element_type=jnp.float32)
                    new.append((new_max, weighted * jnp.exp2(row_max - new_max) + update))
                return tuple(new)

            initial = (
                jnp.full((2 * half, 1), neg_large, jnp.float32),
                jnp.zeros((2 * half, 2 * HEAD_DIM), jnp.float32),
            )
            state = lax.fori_loop(0, s + 1, step, (initial, initial))
            for i in range(2):
                weighted = state[i][1]
                value = (weighted[:, :HEAD_DIM] / weighted[:, HEAD_DIM:]).astype(jnp.bfloat16)
                for part in range(2):
                    lane = pl.multiple_of((4 * quad + 2 * i + part) * HEAD_DIM, HEAD_DIM)
                    attended[side, :, pl.ds(lane, HEAD_DIM)] = value[part * half : (part + 1) * half]

    def mixed(side, pos, t):
        m = side * passes + pos * tiles + t
        w_copy(m).wait()
        value = jnp.dot(attended[side], weights[lax.rem(m, slots)], preferred_element_type=jnp.float32)

        @pl.when(m + slots < 2 * passes)
        def _():
            w_copy(m + slots).start()

        return value

    def copy1(side, slot, t):
        return pltpu.make_async_remote_copy(
            send1.at[side, slot, t], recv1.at[side, slot, t], ss1.at[side, slot, t], rs1.at[side, slot, t],
            device_id=(first_peer(t), s), device_id_type=MESH,
        )

    def copy2(side, t):
        return pltpu.make_async_remote_copy(
            send2.at[side, t], recv2.at[side, t], ss2.at[side, t], rs2.at[side, t],
            device_id=(second_peer(t), s), device_id_type=MESH,
        )

    def send_out(side):
        @pl.loop(0, 2 * tiles)
        def _(m):
            slot, t = m // tiles, lax.rem(m, tiles)
            send1[side, slot, t] = mixed(side, slot, t).astype(jnp.bfloat16)
            copy1(side, slot, t).start()

    def pass_on(side):
        @pl.loop(0, tiles)
        def _(t):
            kept[side, t] = mixed(side, 2, t)

        @pl.loop(0, tiles)
        def _(t):
            value = mixed(side, 3, t)
            copy1(side, 0, t).wait_recv()
            send2[side, t] = (value + recv1[side, 0, t].astype(jnp.float32)).astype(jnp.bfloat16)
            copy2(side, t).start()

    def collect(side):
        @pl.loop(0, tiles)
        def _(t):
            copy1(side, 1, t).wait_recv()
            copy2(side, t).wait_recv()
            value = kept[side, t] + recv1[side, 1, t].astype(jnp.float32) + recv2[side, t].astype(jnp.float32)
            mine = pl.ds(pl.multiple_of(side * half, half), half)
            out_ref[mine, pl.ds(pl.multiple_of(t * wide, wide), wide)] = value.astype(jnp.bfloat16)

    def primary(kk):
        @pl.when(low)
        def _():
            up_stage(kk)

        @pl.when(jnp.logical_not(low))
        def _():
            dn_stage(kk)

    def secondary(kk):
        @pl.when(low)
        def _():
            dn_stage(kk)

        @pl.when(jnp.logical_not(low))
        def _():
            up_stage(kk)

    def wait_primary(kk):
        @pl.when(low)
        def _():
            wait_up_sends(kk)

        @pl.when(jnp.logical_not(low))
        def _():
            wait_dn_sends(kk)

    def wait_secondary(kk):
        @pl.when(low)
        def _():
            wait_dn_sends(kk)

        @pl.when(jnp.logical_not(low))
        def _():
            wait_up_sends(kk)

    pair_stage(0)
    for i in range(1, n):
        id_copy(i).start()

    @pl.loop(0, chunks)
    def _(kk):
        @pl.when(kk >= 2)
        def _():
            wait_primary(kk - 2)

        primary(kk)

        @pl.when(kk + 1 < chunks)
        def _():
            pair_stage(kk + 1)

        @pl.when(kk >= 1)
        def _():
            secondary(kk - 1)

        @pl.when(kk == 1)
        def _():
            angles = (s * rows + lax.broadcasted_iota(jnp.int32, (rows, HEAD_DIM), 0)).astype(
                jnp.float32
            ) * freq_ref[...]
            lane = lax.broadcasted_iota(jnp.int32, (rows, HEAD_DIM), 1)
            sine = jnp.sin(angles)
            cos_ref[...] = jnp.cos(angles)
            sin_ref[...] = jnp.where(lane < HEAD_DIM // 2, -sine, sine)

        @pl.when(kk >= 2)
        def _():
            finish(kk - 2)

    for i in range(1, n):
        id_copy(i).wait_send()
        id_wait(i).wait_recv()

    @pl.loop(1, line)
    def _(h):
        relay(h)

    @pl.loop(0, z + 1)
    def _(zz):
        kv_pair_wait(zz).wait_recv()

    @pl.loop(0, 2)
    def _(side):
        attend(side)
        send_out(side)

        @pl.when(side == 0)
        def _():
            secondary(chunks - 1)
            finish(chunks - 2)

        pass_on(side)

        @pl.when(side == 0)
        def _():
            finish(chunks - 1)

    @pl.loop(0, 2)
    def _(side):
        collect(side)

    @pl.loop(0, chunks)
    def _(kk):
        @pl.when(kk >= chunks - 2)
        def _():
            wait_primary(kk)

            @pl.loop(0, line)
            def _(dest):
                pair_copy(kk, dest).wait_send()

        wait_secondary(kk)

    @pl.loop(0, z + 1)
    def _(zz):
        kv_pair(zz).wait_send()

        @pl.when(z < line - 1)
        def _():
            kv_line(zz).wait_send()

    @pl.loop(0, 2)
    def _(side):
        @pl.loop(0, tiles)
        def _(t):
            copy1(side, 0, t).wait_send()
            copy1(side, 1, t).wait_send()
            copy2(side, t).wait_send()


def body(seq, groups, tokens, proj_weight, proj_bias, out_weight, doc_ids):
    rows = doc_ids.shape[0]
    columns = proj_weight.shape[1]
    width = 2 * HEAD_DIM
    chunks = columns // width
    line = seq // 2
    half = rows // 2
    q_width = GQA * HEAD_DIM
    block = out_weight.shape[1] // groups
    wide = 4 * HEAD_DIM
    tiles = block // wide
    slots = 2 * tiles
    inverse_freq = theta_base ** (-(jnp.arange(HEAD_DIM // 2, dtype=jnp.float32) * 2.0) / HEAD_DIM)
    freq = jnp.concatenate([inverse_freq, inverse_freq])[None, :]
    vmem = pl.BlockSpec(memory_space=pltpu.VMEM)
    dma = pltpu.SemaphoreType.DMA
    bf16, f32, i32 = jnp.bfloat16, jnp.float32, jnp.int32

    return pl.pallas_call(
        functools.partial(layer_kernel, line, chunks, rows, width, groups, tiles, wide, slots),
        out_shape=jax.ShapeDtypeStruct((rows, block), bf16),
        in_specs=[vmem] * 5 + [pl.BlockSpec(memory_space=pl.ANY)],
        out_specs=vmem,
        scratch_shapes=[
            pltpu.VMEM((2, line, rows, width), bf16),
            pltpu.VMEM((chunks, line, rows, width), bf16),
            pltpu.VMEM((chunks, line, rows, width), bf16),
            pltpu.VMEM((chunks, line, rows, width), bf16),
            pltpu.VMEM((rows, width), f32),
            pltpu.VMEM((2, GQA * half, HEAD_DIM), bf16),
            pltpu.VMEM((seq, rows, width), bf16),
            pltpu.VMEM((2, half, q_width), bf16),
            pltpu.VMEM((8, rows), i32),
            pltpu.VMEM((rows, HEAD_DIM), i32),
            pltpu.VMEM((seq, 8, rows), i32),
            pltpu.VMEM((8, columns), f32),
            pltpu.VMEM((rows, HEAD_DIM), f32),
            pltpu.VMEM((rows, HEAD_DIM), f32),
            pltpu.VMEM((slots, q_width, wide), bf16),
            pltpu.VMEM((2, tiles, half, wide), f32),
            pltpu.VMEM((2, 2, tiles, half, wide), bf16),
            pltpu.VMEM((2, 2, tiles, half, wide), bf16),
            pltpu.VMEM((2, tiles, half, wide), bf16),
            pltpu.VMEM((2, tiles, half, wide), bf16),
        ]
        + [dma((chunks, line))] * 5
        + [dma((seq,))] * 2
        + [dma((line,))] * 4
        + [dma((slots,)), dma((2, 2, tiles)), dma((2, 2, tiles)), dma((2, tiles)), dma((2, tiles))],
        compiler_params=pltpu.CompilerParams(
            collective_id=0, has_side_effects=True, vmem_limit_bytes=67043328
        ),
        name="layer",
    )(tokens, proj_weight, proj_bias[None, :], freq, doc_ids[None, :], out_weight)


def solution(mesh):
    return jax.shard_map(
        functools.partial(body, mesh.shape["seq"], mesh.shape["grp"]),
        mesh=mesh,
        in_specs=(P(None, "seq"), P("seq", "grp"), P("grp"), P("grp", None), P("seq")),
        out_specs=P("seq", "grp"),
        check_vma=False,
    )
```
